256 devices in a mesh: dp: 4 (over y_lo, core), sp: 8 (over y_hi, x), tp: 8 (over z).
Axes of the slice: x: 4, y: 4 (y_hi: 2, y_lo: 2; y = y_hi * 2 + y_lo), z: 8, core: 2. Of those that a mesh axis runs over, the one named last changes fastest.
Arguments:
- query: bfloat16 [4, 3072, 3072], P('dp', 'sp', 'tp'), may hold values from -110 to 110
- key: bfloat16 [4, 3072, 3072], P('dp', 'sp', 'tp'), may hold values from -8 to 8
- value: bfloat16 [4, 3072, 3072], P('dp', 'sp', 'tp'), may hold values from -6 to 6
- text_key: bfloat16 [4, 256, 3072], P('dp', None, 'tp'), may hold values from -6 to 6
- text_value: bfloat16 [4, 256, 3072], P('dp', None, 'tp'), may hold values from -6 to 6
- grad_out: bfloat16 [4, 3072, 3072], P('dp', 'sp', 'tp'), may hold values from -6 to 6
- gate: bfloat16 [4, 3072], P('dp'), may hold values from 0.5 to 1.5
- out_weight: bfloat16 [3072, 3072], P('tp', 'dp'), may hold values from -0.109375 to 0.109375
- windows: int32 [8, 2], P('sp'), may hold values from 0 to 2, as said below
- tile_map: int32 [8, 1], replicated, may hold values from 0 to 2, as said below
- text_count: int32 [4], P('dp'), may hold values from 1 to 256
Outputs:
- grad_query: bfloat16 [4, 3072, 3072], P('dp', 'sp', 'tp')
- grad_key: bfloat16 [4, 3072, 3072], P('dp', 'sp', 'tp')
- grad_value: bfloat16 [4, 3072, 3072], P('dp', 'sp', 'tp')
- grad_text_key: bfloat16 [4, 256, 3072], P('dp', None, 'tp')
- grad_text_value: bfloat16 [4, 256, 3072], P('dp', None, 'tp')
- grad_weight: float32 [3072, 3072], P('tp', 'dp')
The draws below stay inside these ranges and needn't reach their ends.
Inputs may be any that keep to these rules, and one draw needn't show every extreme that they name: `tile_map`: the positions within each row are distinct. `windows`: the time reach is 0 or 1; the first tile of every time slab has time reach 1 and spatial reach 2.
All inputs are finite; a program needn't handle non-finite values.
Results may differ from the reference program's by a relative error of at most 0.024.
Values may be sent and summed in bfloat16 or wider, within the bound.
No kernel may reach another device: no remote copies, remote signals or barrier semaphores. Data moves between devices by JAX's collectives and lax.ppermute only.
A program may use at most 64 MiB of HBM per device.

```python
import jax
import jax.numpy as jnp
from jax import lax

D = 3072
HD = 128
TILE = 384
TILES_DEV = 1
TXT = 256
VTOK = 3072
SAMPLES = 4
NTILES = 8
N_SP = 8


def base_keys(key):
    raw = jax.random.normal(jax.random.fold_in(key, 11), (SAMPLES, VTOK, D), jnp.float32)
    return jnp.clip(raw, -6.0, 6.0)


def draw_key(key, part):
    keys = base_keys(key)
    return keys.astype(jnp.bfloat16)


def draw_query(key, part):
    fresh = jnp.clip(jax.random.normal(jax.random.fold_in(key, 13), (SAMPLES, VTOK, D), jnp.float32), -6.0, 6.0)
    return fresh.astype(jnp.bfloat16)


def draw_tile_map(key, part):
    streams = jax.random.split(jax.random.fold_in(key, 21), N_SP)
    orders = jax.vmap(lambda stream: jax.random.permutation(stream, 3 * TILES_DEV)[:TILES_DEV])(streams)
    orders = orders.astype(jnp.int32)
    highest = 3 * TILES_DEV - 1
    first_row = orders[0]
    has_lowest = jnp.any(first_row == 0)
    first_row = first_row.at[0].set(jnp.where(has_lowest, first_row[0], 0))
    orders = orders.at[0].set(first_row)
    last_row = orders[N_SP - 1]
    has_highest = jnp.any(last_row == highest)
    last_row = last_row.at[0].set(jnp.where(has_highest, last_row[0], highest))
    orders = orders.at[N_SP - 1].set(last_row)
    return orders.astype(jnp.int32)


def draw_windows(key, part):
    time_reach = jax.random.randint(jax.random.fold_in(key, 31), (NTILES,), 0, 2)
    space_reach = jax.random.randint(jax.random.fold_in(key, 32), (NTILES,), 0, 3 * TILES_DEV)
    first = jnp.arange(NTILES) % TILES_DEV == 0
    time_reach = jnp.where(first, 1, time_reach)
    space_reach = jnp.where(first, 3 * TILES_DEV - 1, space_reach)
    return jnp.stack([time_reach, space_reach], axis=1).astype(jnp.int32)


def place_ends(result, stream_key, least, top_value):
    longest = result.shape.index(max(result.shape))
    spots = []
    for shift in (0, 1):
        where = [jax.random.randint(jax.random.fold_in(stream_key, axis), (), 0, length) for axis, length in enumerate(result.shape)]
        where[longest] = (where[longest] + shift) % result.shape[longest]
        spots.append(tuple(where))
    return result.at[spots[0]].set(least).at[spots[1]].set(top_value)


def steps_of(own_key, shape, cuts, low, largest):
    level = 1.0
    for position, blocks in cuts:
        steps = jax.random.uniform(jax.random.fold_in(jax.random.fold_in(own_key, 6), position), (blocks,), jnp.float32, low / len(cuts), largest / len(cuts))
        level = level * jnp.repeat(jnp.exp(steps), shape[position] // blocks).reshape((-1,) + (1,) * (len(shape) - 1 - position))
    return level


def normal_values(own_key, dims, width, most, cuts=(), held_as=jnp.bfloat16):
    values = width * jax.random.normal(own_key, dims, jnp.float32)
    if cuts:
        values = values * steps_of(own_key, dims, cuts, -0.22, 0.18)
    return jnp.clip(values, -most, most).astype(held_as)


def setup_inputs(seed: int = 0) -> dict:
    streams_of = jax.random.split(jax.random.key(seed), 12)
    return {
        "query": draw_query(jax.random.fold_in(streams_of[11], 71), 0),
        "key": draw_key(jax.random.fold_in(streams_of[11], 71), 0),
        "value": normal_values(streams_of[2], (SAMPLES, VTOK, D), 1.0, 6.0, ((0, 4), (1, 8), (2, 8))),
        "text_key": normal_values(streams_of[3], (SAMPLES, TXT, D), 1.0, 6.0, ((0, 4), (2, 8))),
        "text_value": normal_values(streams_of[4], (SAMPLES, TXT, D), 1.0, 6.0, ((0, 4), (2, 8))),
        "grad_out": normal_values(streams_of[5], (SAMPLES, VTOK, D), 1.0, 6.0, ((0, 4), (1, 8), (2, 8))),
        "gate": jnp.clip(0.5 + 1.0 * jax.random.uniform(streams_of[6], (SAMPLES, D), jnp.float32) ** steps_of(streams_of[6], (SAMPLES, D), ((0, 4),), -0.2, 0.2), 0.5, 1.5).astype(jnp.bfloat16),
        "out_weight": normal_values(streams_of[7], (D, D), D ** -0.5, 0.109375, ((0, 8), (1, 4))),
        "windows": draw_windows(jax.random.fold_in(streams_of[11], 71), 0),
        "tile_map": draw_tile_map(jax.random.fold_in(streams_of[11], 71), 0),
        "text_count": place_ends(jax.random.randint(streams_of[10], (SAMPLES,), 1, TXT + 1), jax.random.fold_in(streams_of[10], 1), 1, TXT).astype(jnp.int32),
    }


def window_mask(own_map, side_maps, valid, spans, text_live):
    reach = jnp.abs(jnp.arange(3, dtype=jnp.int32) - 1)
    near_time = reach[None, :, None] <= spans[:, 0][:, None, None]
    near_space = jnp.abs(own_map[:, None, None] - side_maps[None, :, :]) <= spans[:, 1][:, None, None]
    allowed = near_time & near_space & valid[None, :, None]
    count = own_map.shape[0]
    tiles = allowed.reshape(count, 3 * count)
    video = jnp.broadcast_to(tiles[:, None, :, None], (count, TILE, 3 * count, TILE))
    video = video.reshape(count * TILE, 3 * count * TILE)
    text = jnp.broadcast_to(text_live[None, :], (count * TILE, text_live.shape[0]))
    return jnp.concatenate([video, text], axis=1)


def tile_attention(query, keys, values, grad_attn, allowed):
    factor = HD ** -0.5
    scores = factor * jnp.dot(query, keys.T, preferred_element_type=jnp.float32)
    scores = jnp.where(allowed, scores, -1e30)
    top = jnp.max(scores, axis=1, keepdims=True)
    weights = jnp.exp(scores - top)
    weights = weights / jnp.sum(weights, axis=1, keepdims=True)
    probs = weights.astype(jnp.bfloat16)
    attended = jnp.dot(probs, values, preferred_element_type=jnp.float32).astype(jnp.bfloat16)
    delta = jnp.sum(grad_attn.astype(jnp.float32) * attended.astype(jnp.float32), axis=1, keepdims=True)
    grad_probs = jnp.dot(grad_attn, values.T, preferred_element_type=jnp.float32)
    grad_scores = (weights * (grad_probs - delta)).astype(jnp.bfloat16)
    grad_query = factor * jnp.dot(grad_scores, keys, preferred_element_type=jnp.float32)
    grad_keys = factor * jnp.dot(grad_scores.T, query, preferred_element_type=jnp.float32)
    grad_values = jnp.dot(probs.T, grad_attn, preferred_element_type=jnp.float32)
    return attended, grad_query, grad_keys, grad_values


def gather_back(parts, slabs, tok):
    video = parts[:, :3 * tok].reshape(slabs, 3, tok, HD)
    empty = jnp.zeros((1, tok, HD), jnp.float32)
    total = video[:, 1] + jnp.concatenate([video[1:, 0], empty], axis=0)
    total = total + jnp.concatenate([empty, video[:-1, 2]], axis=0)
    return total.reshape(slabs * tok, HD), jnp.sum(parts[:, 3 * tok:], axis=0)


def reference(query, key, value, text_key, text_value, grad_out, gate, out_weight, windows, tile_map, text_count):
    slabs = N_SP
    tok = TILE * TILES_DEV
    heads = D // HD
    blank = jnp.zeros((1, TILES_DEV), jnp.int32)
    padded_map = jnp.concatenate([blank, tile_map.astype(jnp.int32), blank], axis=0)
    weight_grad = jnp.zeros((D, D), jnp.float32)
    outs = [[], [], [], [], []]
    for sample in range(SAMPLES):
        scaled = (grad_out[sample].astype(jnp.float32) * gate[sample].astype(jnp.float32)[None, :]).astype(jnp.bfloat16)
        grad_attn = jnp.dot(scaled, out_weight.T, preferred_element_type=jnp.float32).astype(jnp.bfloat16)
        text_live = jnp.arange(TXT, dtype=jnp.int32) < text_count[sample]

        def one_head(head):
            start = (head * HD).astype(jnp.int32)

            def cut(array):
                return lax.dynamic_slice_in_dim(array, start, HD, 1)

            queries = cut(query[sample]).reshape(slabs, tok, HD)
            grads = cut(grad_attn).reshape(slabs, tok, HD)
            zero_slab = jnp.zeros((1, tok, HD), jnp.bfloat16)
            keys = jnp.concatenate([zero_slab, cut(key[sample]).reshape(slabs, tok, HD), zero_slab], axis=0)
            vals = jnp.concatenate([zero_slab, cut(value[sample]).reshape(slabs, tok, HD), zero_slab], axis=0)
            text_k = cut(text_key[sample])
            text_v = cut(text_value[sample])

            def one_slab(slab):
                slab = slab.astype(jnp.int32)
                near_k = lax.dynamic_slice_in_dim(keys, slab, 3, 0).reshape(3 * tok, HD)
                near_v = lax.dynamic_slice_in_dim(vals, slab, 3, 0).reshape(3 * tok, HD)
                all_k = jnp.concatenate([near_k, text_k], axis=0)
                all_v = jnp.concatenate([near_v, text_v], axis=0)
                own_map = lax.dynamic_index_in_dim(tile_map.astype(jnp.int32), slab, 0, keepdims=False)
                side_maps = lax.dynamic_slice_in_dim(padded_map, slab, 3, 0)
                others = slab + jnp.arange(3, dtype=jnp.int32) - 1
                valid = (others >= 0) & (others < slabs)
                spans = lax.dynamic_slice_in_dim(windows.astype(jnp.int32), slab * TILES_DEV, TILES_DEV, 0)
                allowed = window_mask(own_map, side_maps, valid, spans, text_live)
                qs = lax.dynamic_index_in_dim(queries, slab, 0, keepdims=False)
                gs = lax.dynamic_index_in_dim(grads, slab, 0, keepdims=False)
                return tile_attention(qs, all_k, all_v, gs, allowed)

            attended, grad_q, grad_k, grad_v = lax.map(one_slab, jnp.arange(slabs, dtype=jnp.int32))
            video_k, text_gk = gather_back(grad_k, slabs, tok)
            video_v, text_gv = gather_back(grad_v, slabs, tok)
            return attended.reshape(slabs * tok, HD), grad_q.reshape(slabs * tok, HD), video_k, video_v, text_gk, text_gv

        results = lax.map(one_head, jnp.arange(heads, dtype=jnp.int32))

        def joined(stacked):
            return jnp.transpose(stacked, (1, 0, 2)).reshape(stacked.shape[1], D)

        attended = joined(results[0])
        weight_grad = weight_grad + jnp.dot(attended.T, scaled, preferred_element_type=jnp.float32)
        for place in range(5):
            outs[place].append(joined(results[place + 1]).astype(jnp.bfloat16))
    stacked = [jnp.stack(items, axis=0) for items in outs]
    return stacked[0], stacked[1], stacked[2], stacked[3], stacked[4], weight_grad
```

```python
import jax
import jax.numpy as jnp
from jax import lax
from jax.experimental import pallas as pl
from jax.experimental.pallas import tpu as pltpu
from jax.sharding import Mesh, PartitionSpec as P

HD = 128
B16 = jnp.bfloat16
F32 = jnp.float32
NEG = -1e30
LOG2E = 1.4426950408889634

VM = pltpu.MemorySpace.VMEM
SM = pltpu.MemorySpace.SMEM


def vspec():
    return pl.BlockSpec(memory_space=VM)


def sspec():
    return pl.BlockSpec(memory_space=SM)


def nn(a, b):
    return lax.dot_general(a, b, (((1,), (0,)), ((), ())), preferred_element_type=F32)


def nt(a, b):
    return lax.dot_general(a, b, (((1,), (1,)), ((), ())), preferred_element_type=F32)


def ring(count, step):
    return [(i, (i + step) % count) for i in range(count)]


def forward_kernel(flags, q, kown, vown, prev, nxt, tk, tv, probs, att_t):
    tok, width = q.shape
    txt = tk.shape[0]
    factor = HD ** (-0.5) * LOG2E
    for h in range(width // HD):
        cols = slice(h * HD, (h + 1) * HD)
        qh = q[:, cols]
        keys = [prev[0, :, cols], kown[:, cols], nxt[0, :, cols]]
        scores = []
        for place in range(3):
            s = nt(keys[place], qh)
            scores.append(jnp.where(flags[place] != 0, s, NEG))
        s = nt(tk[:, cols], qh)
        live = lax.broadcasted_iota(jnp.int32, (txt, tok), 0) < flags[3]
        scores.append(jnp.where(live, s, NEG))
        top = scores[0].max(axis=0, keepdims=True)
        for s in scores[1:]:
            top = jnp.maximum(top, s.max(axis=0, keepdims=True))
        shift = top * factor
        total = jnp.zeros((1, tok), F32)
        expd = []
        for s in scores:
            e = jnp.exp2(s * factor - shift)
            total = total + e.sum(axis=0, keepdims=True)
            expd.append(e)
        inverse = 1.0 / total
        values = [prev[1, :, cols], vown[:, cols], nxt[1, :, cols], tv[:, cols]]
        out = jnp.zeros((HD, tok), F32)
        row = 0
        for e, v in zip(expd, values):
            p = (e * inverse).astype(B16)
            probs[h, row : row + p.shape[0], :] = p
            row += p.shape[0]
            out = out + nn(v.T, p)
        att_t[cols, :] = out.astype(B16)


def forward(flags, q, kown, vown, prev, nxt, tk, tv):
    tok, width = q.shape
    keys = 3 * tok + tk.shape[0]
    return pl.pallas_call(
        forward_kernel,
        out_shape=(
            jax.ShapeDtypeStruct((width // HD, keys, tok), B16),
            jax.ShapeDtypeStruct((width, tok), B16),
        ),
        in_specs=[sspec()] + [vspec()] * 7,
        out_specs=(vspec(), vspec()),
        name="attn_fwd",
    )(flags, q, kown, vown, prev, nxt, tk, tv)


def contract_shard(flags, block, shard, gate, w_near, w_far, att_t, lw):
    side = block & 1
    owner = block >> 1
    diff = owner ^ flags[5]
    across = diff >> 1
    scaled = (shard.astype(F32) * gate[block].astype(F32)).astype(B16)
    w = jnp.where((diff & 1) == 0, w_near[across, side], w_far[across, side])
    part = nn(att_t, scaled).astype(B16)
    lw[diff & 1, owner >> 1, side] = part
    return nt(w, scaled)


def early_kernel(flags, s0, s1, s2, s3, s4, gate, w_near, w_far, att, acc, lw):
    t = flags[4]
    att_t = att[...]
    total = None
    for step, ref in ((0, s0), (7, s1), (1, s2), (6, s3), (2, s4)):
        part = contract_shard(flags, (t + step) & 7, ref[...], gate, w_near, w_far, att_t, lw)
        total = part if total is None else total + part
    acc[...] = total


def late_kernel(flags, s5, s6, s7a, s7b, gate, w_near, w_far, att, acc, lw_in, ga, lw):
    lw[...] = lw_in[...]
    t = flags[4]
    att_t = att[...]
    total = acc[...]
    total = total + contract_shard(flags, (t + 5) & 7, s5[...], gate, w_near, w_far, att_t, lw)
    total = total + contract_shard(flags, (t + 3) & 7, s6[...], gate, w_near, w_far, att_t, lw)
    both = jnp.concatenate([s7a[...], s7b[...]], axis=0)
    total = total + contract_shard(flags, (t + 4) & 7, both, gate, w_near, w_far, att_t, lw)
    ga[...] = total.astype(B16)


def early(flags, shards, gate, w_near, w_far, att_t):
    tok = shards[0].shape[0]
    width = att_t.shape[0]
    return pl.pallas_call(
        early_kernel,
        out_shape=(
            jax.ShapeDtypeStruct((width, tok), F32),
            jax.ShapeDtypeStruct((2, 2, 2, width, shards[0].shape[1]), B16),
        ),
        in_specs=[sspec()] + [vspec()] * 9,
        out_specs=(vspec(), vspec()),
        name="contract_early",
    )(flags, *shards, gate, w_near, w_far, att_t)


def late(flags, shards, gate, w_near, w_far, att_t, acc, lw):
    tok = shards[0].shape[0]
    width = att_t.shape[0]
    return pl.pallas_call(
        late_kernel,
        out_shape=(
            jax.ShapeDtypeStruct((width, tok), B16),
            jax.ShapeDtypeStruct(lw.shape, lw.dtype),
        ),
        in_specs=[sspec()] + [vspec()] * 10,
        out_specs=(vspec(), vspec()),
        input_output_aliases={10: 1},
        name="contract_late",
    )(flags, *shards, gate, w_near, w_far, att_t, acc, lw)


def piece_grads(p_t, key, value, qh, ga_t, ga, delta):
    grad_p = nn(value, ga_t)
    ds_t = (p_t.astype(F32) * (grad_p - delta)).astype(B16)
    factor = HD ** (-0.5)
    return ds_t, factor * nn(ds_t, qh), nn(p_t, ga)


def backward_kernel(
    q, kown, vown, prev, nxt, tk, tv, probs, att, gat, gq, gprev, gown, gnext, gtext
):
    tok, width = q.shape
    factor = HD ** (-0.5)
    for h in range(width // HD):
        cols = slice(h * HD, (h + 1) * HD)
        qh = q[:, cols]
        ga_t = gat[cols, :]
        ga = ga_t.T
        delta = jnp.sum(ga_t.astype(F32) * att[cols, :].astype(F32), axis=0, keepdims=True)
        pieces = (
            (3 * tok, tk[:, cols], tv[:, cols], gtext),
            (0, prev[0, :, cols], prev[1, :, cols], gprev),
            (2 * tok, nxt[0, :, cols], nxt[1, :, cols], gnext),
            (tok, kown[:, cols], vown[:, cols], gown),
        )
        gq_t = jnp.zeros((HD, tok), F32)
        for row, key, value, out in pieces:
            p_t = probs[h, row : row + key.shape[0], :]
            ds_t, gk, gv = piece_grads(p_t, key, value, qh, ga_t, ga, delta)
            out[0, :, cols] = gk.astype(out.dtype)
            out[1, :, cols] = gv.astype(out.dtype)
            gq_t = gq_t + nn(key.T, ds_t)
        gq[:, cols] = (factor * gq_t).T.astype(B16)


def backward(q, kown, vown, prev, nxt, tk, tv, probs, att_t, ga_t):
    tok, width = q.shape
    txt = tk.shape[0]
    return pl.pallas_call(
        backward_kernel,
        out_shape=(
            jax.ShapeDtypeStruct((tok, width), B16),
            jax.ShapeDtypeStruct((2, tok, width), B16),
            jax.ShapeDtypeStruct((2, tok, width), F32),
            jax.ShapeDtypeStruct((2, tok, width), B16),
            jax.ShapeDtypeStruct((2, txt, width), B16),
        ),
        in_specs=[vspec()] * 10,
        out_specs=(vspec(),) * 5,
        name="attn_bwd",
    )(q, kown, vown, prev, nxt, tk, tv, probs, att_t, ga_t)


def visibility(windows, tile_map, text_count, index, slabs):
    padded = jnp.concatenate([tile_map[:1], tile_map, tile_map[:1]], axis=0)
    side = lax.dynamic_slice_in_dim(padded, index, 3, 0)[:, 0]
    own = side[1]
    offset = jnp.arange(3, dtype=jnp.int32) - 1
    others = index + offset
    allowed = (
        (jnp.abs(offset) <= windows[0, 0])
        & (jnp.abs(own - side) <= windows[0, 1])
        & (others >= 0)
        & (others < slabs)
    )
    return allowed.astype(jnp.int32)


def per_device(
    query, key, value, text_key, text_value, grad_out, gate, out_weight, windows, tile_map, text_count
):
    sp = lax.axis_size("sp")
    tp = lax.axis_size("tp")
    tok, width = query.shape[1], query.shape[2]
    txt = text_key.shape[1]
    rows = out_weight.shape[0]
    index = lax.axis_index("sp")
    dp_index = lax.axis_index("dy") * 2 + lax.axis_index("dc")
    flags = jnp.concatenate(
        [
            visibility(windows, tile_map, text_count, index, sp),
            text_count,
            lax.axis_index("tp")[None],
            dp_index[None],
        ]
    ).astype(jnp.int32)

    own = grad_out[0]
    right = [own]
    left = [own]
    for _ in range(3):
        right.append(lax.ppermute(right[-1], "tp", ring(tp, 1)))
        left.append(lax.ppermute(left[-1], "tp", ring(tp, -1)))
    half = tok // 2
    last_a = lax.ppermute(right[3][:half], "tp", ring(tp, 1))
    last_b = lax.ppermute(left[3][half:], "tp", ring(tp, -1))

    pair = jnp.stack([key[0], value[0]], axis=0)
    prev = lax.ppermute(pair, "sp", [(i, i + 1) for i in range(sp - 1)])
    nxt = lax.ppermute(pair, "sp", [(i + 1, i) for i in range(sp - 1)])

    w_own = jnp.swapaxes(out_weight.reshape(rows, 2, -1), 0, 1)
    w_across = lax.ppermute(w_own, "dy", [(0, 1), (1, 0)])
    w_near = jnp.stack([w_own, w_across], axis=0)
    w_far = lax.ppermute(w_near, "dc", [(0, 1), (1, 0)])
    gates = gate[0].reshape(tp, 1, -1)

    q, k, v, tk, tv = query[0], key[0], value[0], text_key[0], text_value[0]
    probs, att_t = forward(flags, q, k, v, prev, nxt, tk, tv)
    acc, lw = early(
        flags, (own, right[1], left[1], right[2], left[2]), gates, w_near, w_far, att_t
    )
    ga_t, lw = late(
        flags, (right[3], left[3], last_a, last_b), gates, w_near, w_far, att_t, acc, lw
    )

    other = lax.ppermute(lw[1], "dc", [(0, 1), (1, 0)])
    lw2 = (lw[0].astype(F32) + other.astype(F32)).astype(B16)
    cut = rows // sp
    lw2 = lw2.reshape(2, 2, sp, cut, -1)
    lw2 = jnp.transpose(lw2, (0, 2, 1, 3, 4)).reshape(2 * sp, 2, cut, -1)
    lw_in = lax.all_to_all(lw2, ("dy", "sp"), 0, 0, tiled=True)
    lw_sum = jnp.sum(lw_in.astype(F32), axis=0).astype(B16)

    gq, gprev, gown, gnext, gtext = backward(q, k, v, prev, nxt, tk, tv, probs, att_t, ga_t)

    tcut = txt // sp
    text_parts = jnp.swapaxes(gtext.reshape(2, sp, tcut, width), 0, 1)
    text_in = lax.all_to_all(text_parts, "sp", 0, 0, tiled=True)
    text_sum = jnp.sum(text_in.astype(F32), axis=0).astype(B16)

    from_later = lax.ppermute(gprev, "sp", [(i + 1, i) for i in range(sp - 1)])
    from_earlier = lax.ppermute(gnext, "sp", [(i, i + 1) for i in range(sp - 1)])
    total = (gown + from_later.astype(F32) + from_earlier.astype(F32)).astype(B16)

    mine = jnp.concatenate(
        [lw_sum.reshape(2 * cut, width), text_sum.reshape(2 * tcut, width)], axis=0
    )
    copies = jnp.broadcast_to(mine[None], (sp, *mine.shape))
    gathered = lax.all_to_all(copies, "sp", 0, 0, tiled=True)
    weight = gathered[:, : 2 * cut].reshape(sp, 2, cut, width)
    weight = jnp.transpose(weight, (0, 2, 1, 3)).reshape(rows, 2 * width).astype(F32)
    text = gathered[:, 2 * cut :].reshape(sp, 2, tcut, width)
    text_k = text[:, 0].reshape(txt, width)
    text_v = text[:, 1].reshape(txt, width)
    return (
        gq[None],
        total[0][None],
        total[1][None],
        text_k[None],
        text_v[None],
        weight,
    )


def solution(mesh):
    shape = mesh.devices.shape
    fine = Mesh(mesh.devices.reshape(2, shape[0] // 2, *shape[1:]), ("dy", "dc", "sp", "tp"))
    dp = ("dy", "dc")
    placed = (
        P(dp, "sp", "tp"),
        P(dp, "sp", "tp"),
        P(dp, "sp", "tp"),
        P(dp, None, "tp"),
        P(dp, None, "tp"),
        P(dp, "sp", "tp"),
        P(dp, None),
        P("tp", dp),
        P("sp", None),
        P(),
        P(dp),
    )
    return jax.shard_map(
        per_device,
        mesh=fine,
        in_specs=placed,
        out_specs=(
            P(dp, "sp", "tp"),
            P(dp, "sp", "tp"),
            P(dp, "sp", "tp"),
            P(dp, None, "tp"),
            P(dp, None, "tp"),
            P("tp", dp),
        ),
        check_vma=False,
    )
```

```python
import jax
import jax.numpy as jnp
from jax import lax
from jax.experimental import pallas as pl
from jax.experimental.pallas import tpu as pltpu
from jax.sharding import Mesh, PartitionSpec as P


HD = 128
B16 = jnp.bfloat16
F32 = jnp.float32
NEG = -1e30
LOG2E = 1.4426950408889634

VM = pltpu.MemorySpace.VMEM
SM = pltpu.MemorySpace.SMEM


def vspec():
    return pl.BlockSpec(memory_space=VM)


def sspec():
    return pl.BlockSpec(memory_space=SM)


def nn(a, b):
    return lax.dot_general(a, b, (((1,), (0,)), ((), ())), preferred_element_type=F32)


def nt(a, b):
    return lax.dot_general(a, b, (((1,), (1,)), ((), ())), preferred_element_type=F32)


def in_hbm(*arrays):
    return tuple(pltpu.with_memory_space_constraint(array, pltpu.HBM) for array in arrays)


def call(kernel, outs, args, scalars=0, hbm_outs=()):
    return pl.pallas_call(
        kernel,
        out_shape=tuple(
            pltpu.HBM(shape, dtype) if place in hbm_outs else jax.ShapeDtypeStruct(shape, dtype)
            for place, (shape, dtype) in enumerate(outs)
        ),
        in_specs=[sspec()] * scalars + [vspec()] * (len(args) - scalars),
        out_specs=(vspec(),) * len(outs),
        compiler_params=pltpu.CompilerParams(vmem_limit_bytes=16 << 20),
    )(*args)


def ring(count, step):
    return [(i, (i + step) % count) for i in range(count)]


def forward_kernel(windows, tile_map, count, q, kown, vown, prev, nxt, tk, tv, probs, text_probs, att_t):
    tok, width = q.shape
    txt = tk.shape[0]
    slabs = tile_map.shape[0]
    index = lax.axis_index("sp")
    visible = []
    for step in (-1, 0, 1):
        other = index + step
        apart = tile_map[index] - tile_map[jnp.clip(other, 0, slabs - 1)]
        visible.append(
            (abs(step) <= windows[0])
            & (jnp.abs(apart) <= windows[1])
            & (other >= 0)
            & (other < slabs)
        )
    factor = HD ** (-0.5) * LOG2E
    for h in range(width // HD):
        cols = slice(h * HD, (h + 1) * HD)
        qh = q[:, cols]
        keys = [prev[0, :, cols], kown[:, cols], nxt[0, :, cols]]
        scores = [jnp.where(visible[place], nt(keys[place], qh), NEG) for place in range(3)]
        live = lax.broadcasted_iota(jnp.int32, (txt, tok), 0) < count[0]
        scores.append(jnp.where(live, nt(tk[:, cols], qh), NEG))
        top = scores[0].max(axis=0, keepdims=True)
        for s in scores[1:]:
            top = jnp.maximum(top, s.max(axis=0, keepdims=True))
        shift = top * factor
        total = jnp.zeros((1, tok), F32)
        expd = []
        for s in scores:
            e = jnp.exp2(s * factor - shift)
            total = total + e.sum(axis=0, keepdims=True)
            expd.append(e)
        inverse = 1.0 / total
        values = [prev[1, :, cols], vown[:, cols], nxt[1, :, cols], tv[:, cols]]
        out = jnp.zeros((HD, tok), F32)
        for place, (e, v) in enumerate(zip(expd, values)):
            p = (e * inverse).astype(B16)
            if place < 3:
                probs[h, place] = p
            else:
                text_probs[h] = p
            out = out + nn(v.T, p)
        att_t[cols, :] = out.astype(B16)


def block_weight(block, dp, pieces):
    size = pieces[0].shape[1] // 2
    side = pl.multiple_of((block & 1) * size, 128)
    diff = (block >> 1) ^ dp
    near, far, up, down, far_up, far_down = [piece[:, pl.ds(side, size)] for piece in pieces]
    same = (diff & 1) == 0
    low = jnp.where(same, near, far)
    high = jnp.concatenate([jnp.where(same, up, far_up), jnp.where(same, down, far_down)], axis=0)
    return jnp.where(diff < 2, low, high)


def contract_shard(block, shard, gate, pieces, att_t):
    dp = lax.axis_index("dy") * 2 + lax.axis_index("dc")
    scaled = (shard.astype(F32) * gate[block].astype(F32)).astype(B16)
    part = nn(att_t, scaled).astype(B16)
    return nt(block_weight(block, dp, pieces), scaled), part


EARLY = (0, 7, 1, 6, 2)
LATE = (5, 3, 4)


def early_kernel(s0, s1, s2, s3, s4, gate, w0, w1, w2a, w2b, w3a, w3b, att, acc, parts):
    t = lax.axis_index("tp")
    att_t = att[...]
    total = None
    for place, ref in enumerate((s0, s1, s2, s3, s4)):
        grad, part = contract_shard(
            (t + EARLY[place]) & 7, ref[...], gate, (w0, w1, w2a, w2b, w3a, w3b), att_t
        )
        parts[place] = part
        total = grad if total is None else total + grad
    acc[...] = total


def late_kernel(s5, s6, s7a, s7b, gate, w0, w1, w2a, w2b, w3a, w3b, att, acc, parts, ga, keep, send):
    t = lax.axis_index("tp")
    core = lax.axis_index("dc")
    att_t = att[...]
    count, cut = keep.shape[0], keep.shape[3]

    def put(block, part):
        owner = block >> 1
        cells = part.reshape(count, cut, part.shape[1])

        @pl.when((owner & 1) == core)
        def _():
            keep[:, block & 1, owner >> 1] = cells

        @pl.when((owner & 1) != core)
        def _():
            send[:, block & 1, owner >> 1] = cells

    total = acc[...]
    shards = (s5[...], s6[...], jnp.concatenate([s7a[...], s7b[...]], axis=0))
    for step, shard in zip(LATE, shards):
        block = (t + step) & 7
        grad, part = contract_shard(block, shard, gate, (w0, w1, w2a, w2b, w3a, w3b), att_t)
        put(block, part)
        total = total + grad
    for place, step in enumerate(EARLY):
        put((t + step) & 7, parts[place])
    ga[...] = total.astype(B16)


def head_terms(h, q, att, gat):
    cols = slice(h * HD, (h + 1) * HD)
    ga_t = gat[cols, :]
    delta = jnp.sum(ga_t.astype(F32) * att[cols, :].astype(F32), axis=0, keepdims=True)
    return cols, q[:, cols], ga_t, ga_t.T, delta


def piece_grads(p_t, key, value, qh, ga_t, ga, delta):
    grad_p = nn(value, ga_t)
    ds_t = (p_t.astype(F32) * (grad_p - delta)).astype(B16)
    factor = HD ** (-0.5)
    return nn(key.T, ds_t), factor * nn(ds_t, qh), nn(p_t, ga)


def text_kernel(q, tk, tv, probs, att, gat, gtext, gq_t):
    _, width = q.shape
    count, tcut = gtext.shape[0], gtext.shape[1] // 2
    for h in range(width // HD):
        cols, qh, ga_t, ga, delta = head_terms(h, q, att, gat)
        p_t = probs[h]
        dq, gk, gv = piece_grads(p_t, tk[:, cols], tv[:, cols], qh, ga_t, ga, delta)
        gtext[:, :tcut, cols] = gk.astype(B16).reshape(count, tcut, HD)
        gtext[:, tcut:, cols] = gv.astype(B16).reshape(count, tcut, HD)
        gq_t[cols, :] = dq


def video_kernel(q, kown, vown, prev, nxt, probs, att, gat, gq_in, gq, gprev, gown, gnext):
    _, width = q.shape
    factor = HD ** (-0.5)
    for h in range(width // HD):
        cols, qh, ga_t, ga, delta = head_terms(h, q, att, gat)
        gq_t = gq_in[cols, :]
        pieces = (
            (0, prev[0, :, cols], prev[1, :, cols], gprev),
            (2, nxt[0, :, cols], nxt[1, :, cols], gnext),
            (1, kown[:, cols], vown[:, cols], gown),
        )
        for place, key, value, out in pieces:
            p_t = probs[h, place]
            dq, gk, gv = piece_grads(p_t, key, value, qh, ga_t, ga, delta)
            out[0, :, cols] = gk.astype(out.dtype)
            out[1, :, cols] = gv.astype(out.dtype)
            gq_t = gq_t + dq
        gq[:, cols] = (factor * gq_t).T.astype(B16)


def pack_kernel(keep, other, gtext, out):
    rows = keep.shape[1]
    out[:, :rows] = (keep[...].astype(F32) + other[...].astype(F32)).astype(B16)
    out[:, rows:] = gtext[...]


def halo_kernel(own, later, earlier, gk, gv):
    for place, out in enumerate((gk, gv)):
        total = own[place] + later[place].astype(F32) + earlier[place].astype(F32)
        out[...] = total.astype(B16)


def merge_kernel(cells, out):
    count = cells.shape[0]
    cut = cells.shape[1] - out.shape[1]
    span = count // 2
    words = []
    for side in range(2):
        total = cells[side * span, 2 * cut :].astype(F32)
        for place in range(1, span):
            total = total + cells[side * span + place, 2 * cut :].astype(F32)
        words.append(total.astype(B16))
    total = cells[0, : 2 * cut].astype(F32)
    for place in range(1, count):
        total = total + cells[place, : 2 * cut].astype(F32)
    total = total.astype(B16)
    for place in range(count):
        side = place // span
        out[place, :cut] = total[side * cut : (side + 1) * cut]
        out[place, cut:] = words[side]


def unpack_kernel(cells, weight, text_k, text_v):
    count, _, width = cells.shape
    cut = 2 * weight.shape[0] // count
    tcut = text_k.shape[0] // count
    for place in range(count):
        row, col = (place // 2) * cut, (place % 2) * width
        weight[row : row + cut, col : col + width] = cells[place, :cut].astype(F32)
        text_k[place * tcut : (place + 1) * tcut] = cells[place, cut : cut + tcut]
        text_v[place * tcut : (place + 1) * tcut] = cells[place, cut + tcut :]


def y_routes(sp):
    count = sp // 2

    def place(y, x):
        return (y % 2) * sp + (y // 2) * count + x

    spots = [(y, x) for y in range(4) for x in range(count)]
    up = [(place(y, x), place((y + 1) % 4, x)) for y, x in spots]
    down = [(place(y, x), place((y - 1) % 4, x)) for y, x in spots]
    return up, down


def device_program(
    query, key, value, text_key, text_value, grad_out, gate, out_weight, windows, tile_map, text_count
):
    sp = lax.axis_size("sp")
    tp = lax.axis_size("tp")
    tok, width = query.shape[1], query.shape[2]
    txt = text_key.shape[1]
    rows = out_weight.shape[0]
    wide = grad_out.shape[2]
    count = 2 * sp
    cut, tcut = rows // sp, txt // count
    later = [(i, i + 1) for i in range(sp - 1)]
    earlier = [(i + 1, i) for i in range(sp - 1)]
    swap = [(0, 1), (1, 0)]

    own = grad_out[0]
    right = [own]
    left = [own]
    for _ in range(3):
        right.append(lax.ppermute(right[-1], "tp", ring(tp, 1)))
        left.append(lax.ppermute(left[-1], "tp", ring(tp, -1)))
    half = tok // 2
    last_a = lax.ppermute(right[3][:half], "tp", ring(tp, 1))
    last_b = lax.ppermute(left[3][half:], "tp", ring(tp, -1))

    pair = jnp.stack([key[0], value[0]], axis=0)
    prev = lax.ppermute(pair, "sp", later)
    nxt = lax.ppermute(pair, "sp", earlier)

    w0 = out_weight
    w1 = lax.ppermute(w0, "dc", swap)
    up, down = y_routes(sp)
    mid = rows // 2
    w2a = lax.ppermute(w0[:mid], ("dy", "sp"), up)
    w2b = lax.ppermute(w0[mid:], ("dy", "sp"), down)
    w3a = lax.ppermute(w2a, "dc", swap)
    w3b = lax.ppermute(w2b, "dc", swap)
    gates = gate[0].reshape(tp, 1, -1)

    q, k, v, tk, tv = in_hbm(query[0], key[0], value[0], text_key[0], text_value[0])
    (own_hbm, gates, w0) = in_hbm(own, gates, w0)
    probs, text_probs, att_t = call(
        forward_kernel,
        [
            ((width // HD, 3, tok, tok), B16),
            ((width // HD, txt, tok), B16),
            ((width, tok), B16),
        ],
        (windows[0], tile_map.reshape(-1), text_count, q, k, v, prev, nxt, tk, tv),
        scalars=3,
        hbm_outs=(0,),
    )
    acc, parts = call(
        early_kernel,
        [((width, tok), F32), ((len(EARLY), width, own.shape[1]), B16)],
        (own_hbm, right[1], left[1], right[2], left[2], gates, w0, w1, w2a, w2b, w3a, w3b, att_t),
    )
    cells = (count // 2, 2, 2, cut, wide)
    ga_t, keep, send = call(
        late_kernel,
        [((width, tok), B16), (cells, B16), (cells, B16)],
        (right[3], left[3], last_a, last_b, gates, w0, w1, w2a, w2b, w3a, w3b, att_t, acc, parts),
    )

    other = lax.ppermute(send, "dc", swap)
    gtext, gq_t = call(
        text_kernel,
        [((count, 2 * tcut, width), B16), ((width, tok), F32)],
        (q, tk, tv, text_probs, att_t, ga_t),
        hbm_outs=(1,),
    )
    (packed,) = call(
        pack_kernel,
        [((count, 2 * cut + 2 * tcut, wide), B16)],
        (keep.reshape(count, 2 * cut, wide), other.reshape(count, 2 * cut, wide), gtext),
    )
    arrived = lax.all_to_all(packed, ("dy", "sp"), 0, 0, tiled=True)

    gq, gprev, gown, gnext = call(
        video_kernel,
        [
            ((tok, width), B16),
            ((2, tok, width), B16),
            ((2, tok, width), F32),
            ((2, tok, width), B16),
        ],
        (q, k, v, *in_hbm(prev, nxt, probs, att_t, ga_t, gq_t)),
    )
    from_later = lax.ppermute(gprev, "sp", earlier)
    from_earlier = lax.ppermute(gnext, "sp", later)
    total_k, total_v = call(
        halo_kernel, [((tok, width), B16)] * 2, (gown, from_later, from_earlier)
    )

    (copies,) = call(merge_kernel, [((count, cut + 2 * tcut, wide), B16)], (arrived,))
    gathered = lax.all_to_all(copies, ("dy", "sp"), 0, 0, tiled=True)
    weight, text_k, text_v = call(
        unpack_kernel,
        [((rows, 2 * wide), F32), ((txt, width), B16), ((txt, width), B16)],
        (gathered,),
    )
    return (gq[None], total_k[None], total_v[None], text_k[None], text_v[None], weight)


def solution(mesh):
    shape = mesh.devices.shape
    fine = Mesh(mesh.devices.reshape(2, shape[0] // 2, *shape[1:]), ("dy", "dc", "sp", "tp"))
    dp = ("dy", "dc")
    placed = (
        P(dp, "sp", "tp"),
        P(dp, "sp", "tp"),
        P(dp, "sp", "tp"),
        P(dp, None, "tp"),
        P(dp, None, "tp"),
        P(dp, "sp", "tp"),
        P(dp, None),
        P("tp", dp),
        P("sp", None),
        P(),
        P(dp),
    )
    return jax.shard_map(
        device_program,
        mesh=fine,
        in_specs=placed,
        out_specs=(
            P(dp, "sp", "tp"),
            P(dp, "sp", "tp"),
            P(dp, "sp", "tp"),
            P(dp, None, "tp"),
            P(dp, None, "tp"),
            P("tp", dp),
        ),
        check_vma=False,
    )
```
